32 devices in a mesh: expert: 8 (over y, x, core), replica: 4 (over z).
Axes of the slice: x: 2, y: 2, z: 4, core: 2. Of those that a mesh axis runs over, the one named last changes fastest.
Arguments:
- tokens_in: bfloat16 [8192, 2048], P(('expert', 'replica')), may hold values from -6 to 6
- cotangents: bfloat16 [8192, 8192], P(('expert', 'replica')), may hold values from -0.1796875 to 0.1796875
- left_root: bfloat16 [8, 2048, 2048], P('expert'), may hold values from -2 to 6, as said below
- right_root: bfloat16 [8, 8, 1024, 1024], P('expert', 'replica'), may hold values from -2 to 6, as said below
Outputs:
- update: bfloat16 [8, 2048, 8192], P('expert', None, 'replica')
The draws below stay inside these ranges and needn't reach their ends.
Inputs may be any that keep to these rules, and one draw needn't show every extreme that they name: `left_root`: each matrix is symmetric. `right_root`: each block is symmetric.
All inputs are finite; a program needn't handle non-finite values.
Results may differ from the reference program's by a relative error of at most 0.0058.
Values may be sent and summed in bfloat16 or wider, within the bound.
A program may use at most 192 MiB of HBM per device.

```python
import math
import jax
import jax.numpy as jnp
from jax import lax

D = 2048
FF = 8192
BLOCK = 1024
EXPERTS = 8
SLOTS = 32
TOKENS = 8192
BLOCKS = 8


def factor_draw(key, leading, order):
    diag_key, noise_key = jax.random.split(key)
    diagonal = jnp.exp(jax.random.uniform(diag_key, leading + (order,), jnp.float32, 0.0, math.log(3.0)))
    random_part = jnp.clip(jax.random.normal(noise_key, leading + (order, order), jnp.float32), -4.0, 4.0)
    random_part = random_part * (0.8 / math.sqrt(order))
    symmetric = 0.5 * (random_part + jnp.swapaxes(random_part, -1, -2))
    identity = jnp.eye(order, dtype=jnp.float32)
    return (symmetric + identity * diagonal[..., None]).astype(jnp.bfloat16)


def draw_left_root(key, part):
    return factor_draw(jax.random.fold_in(key, 11), (EXPERTS,), D)


def draw_right_root(key, part):
    return factor_draw(jax.random.fold_in(key, 12), (EXPERTS, BLOCKS), BLOCK)


def block_scale(rng, dims, cuts, smallest, top_value):
    loudness = 1.0
    for position, shards_of in cuts:
        steps = jax.random.uniform(jax.random.fold_in(jax.random.fold_in(rng, 6), position), (shards_of,), jnp.float32, smallest / len(cuts), top_value / len(cuts))
        loudness = loudness * jnp.repeat(jnp.exp(steps), dims[position] // shards_of).reshape((-1,) + (1,) * (len(dims) - 1 - position))
    return loudness


def centred(stream_key, dims, spread, most, shards=(), kind=jnp.bfloat16):
    values = jax.random.normal(stream_key, dims, jnp.float32) * spread
    if len(shards) > 0:
        values = block_scale(stream_key, dims, shards, -0.22, 0.18) * values
    return jnp.clip(values, min=-most, max=most).astype(kind)


def setup_inputs(seed: int = 0) -> dict:
    streams_of = jax.random.split(jax.random.key(seed), 5)
    return {
        "tokens_in": centred(streams_of[0], (TOKENS, D), 1.0, 6.0, ((0, 32),)),
        "cotangents": centred(streams_of[1], (TOKENS, FF), 0.03, 0.1796875, ((0, 32),)),
        "left_root": draw_left_root(jax.random.fold_in(streams_of[4], 71), 0),
        "right_root": draw_right_root(jax.random.fold_in(streams_of[4], 71), 0),
    }


def per_expert(inputs):
    expert_tokens, expert_cotangents, left_factor, right_factor = inputs
    gradient = jnp.dot(expert_tokens.T, expert_cotangents, preferred_element_type=jnp.float32).astype(jnp.bfloat16)
    blocks = gradient.reshape(D, BLOCKS, BLOCK).astype(jnp.float32)
    applied = jnp.einsum("dbk,bkj->dbj", blocks, right_factor.astype(jnp.float32))
    applied = applied.astype(jnp.bfloat16).reshape(D, FF)
    return jnp.dot(left_factor, applied, preferred_element_type=jnp.float32).astype(jnp.bfloat16)


def reference(tokens_in, cotangents, left_root, right_root):
    token_groups = jnp.moveaxis(tokens_in.reshape(-1, EXPERTS, SLOTS, D), 1, 0).reshape(EXPERTS, -1, D)
    cotangent_groups = jnp.moveaxis(cotangents.reshape(-1, EXPERTS, SLOTS, FF), 1, 0).reshape(EXPERTS, -1, FF)
    return lax.map(per_expert, (token_groups, cotangent_groups, left_root, right_root))
```

```python
import functools
import jax
import jax.numpy as jnp
from jax import lax
from jax.experimental import pallas as pl
from jax.experimental.pallas import tpu as pltpu
from jax.sharding import PartitionSpec as P


def tile_of(size, most):
    return most if size % most == 0 else size


def route_kernel(
    ne, nr, tok_ref, cot_ref, left_ref, right_ref, x_ref, y_ref,
    tok, cot, left, right, x, y,
    plane_send, up_send, down_send, tok_recv, cot_send, cot_recv, local,
):
    e = lax.axis_index("expert")
    r = lax.axis_index("replica")
    rows = tok_ref.shape[0] // ne
    group = rows * ne
    width = tok.shape[1]
    cols = cot.shape[1]
    blocks, order = right_ref.shape[0], right_ref.shape[1]

    load_left = pltpu.make_async_copy(left_ref, left, local.at[0])
    load_right = pltpu.make_async_copy(right_ref, right, local.at[1])
    load_left.start()
    load_right.start()

    barrier = pltpu.get_barrier_semaphore()

    @pl.loop(1, ne * nr)
    def _(k):
        pl.semaphore_signal(
            barrier, inc=1,
            device_id={"expert": (e + k % ne) % ne, "replica": (r + k // ne) % nr},
        )

    pl.semaphore_wait(barrier, ne * nr - 1)

    def span(origin, source):
        return pl.ds(pl.multiple_of((origin * ne + source) * rows, rows), rows)

    def own_rows(target):
        return pl.ds(pl.multiple_of(target * rows, rows), rows)

    def own_cols(target):
        return pl.ds(pl.multiple_of(target * cols, cols), cols)

    def plane_copy(target):
        return pltpu.make_async_remote_copy(
            tok_ref.at[own_rows(target)], tok.at[span(r, e)],
            plane_send.at[target], tok_recv.at[r * ne + e],
            device_id={"expert": target, "replica": r},
        )

    def relay(origin, source, up):
        at = span(origin, source)
        k = origin * ne + source
        return pltpu.make_async_remote_copy(
            tok.at[at], tok.at[at],
            (up_send if up else down_send).at[k], tok_recv.at[k],
            device_id={"expert": e, "replica": r + 1 if up else r - 1},
        )

    def tok_wait(origin, source):
        pltpu.make_async_remote_copy(
            tok.at[span(origin, source)], tok.at[span(origin, source)],
            up_send.at[0], tok_recv.at[origin * ne + source],
            device_id={"expert": e, "replica": (r + 1) % nr},
        ).wait_recv()

    def cot_copy(te, tr):
        return pltpu.make_async_remote_copy(
            cot_ref.at[own_rows(te), own_cols(tr)], cot.at[span(r, e)],
            cot_send.at[tr * ne + te], cot_recv.at[r * ne + e],
            device_id={"expert": te, "replica": tr},
        )

    def send_cots(te, distance):
        for tr in (r + distance, r - distance):
            @pl.when((tr >= 0) & (tr < nr))
            def _():
                cot_copy(te, tr).start()

    def forward(origin, source, up):
        ahead = (r + 1 < nr) if up else (r > 0)

        @pl.when(ahead)
        def _():
            relay(origin, source, up).start()

    own_tok = pltpu.make_async_copy(tok_ref.at[own_rows(e)], tok.at[span(r, e)], local.at[2])
    own_cot = pltpu.make_async_copy(cot_ref.at[own_rows(e), own_cols(r)], cot.at[span(r, e)], local.at[3])
    own_tok.start()
    own_cot.start()

    @pl.loop(1, ne)
    def _(k):
        plane_copy((e + k) % ne).start()

    own_tok.wait()

    @pl.loop(0, ne)
    def _(k):
        source = (e + ne - k) % ne

        @pl.when(k > 0)
        def _():
            tok_wait(r, source)

        forward(r, source, True)
        forward(r, source, False)
        for distance in range(nr - 1, 1, -1):
            send_cots((e + k) % ne, distance)

    for distance in range(1, nr):
        @pl.loop(0, ne)
        def _(k):
            source = (e + ne - k) % ne

            @pl.when(r - distance >= 0)
            def _():
                tok_wait(r - distance, source)
                forward(r - distance, source, True)

            @pl.when(r + distance < nr)
            def _():
                tok_wait(r + distance, source)
                forward(r + distance, source, False)

            if distance == 1:
                send_cots((e + k) % ne, 1)

                @pl.when(k > 0)
                def _():
                    cot_copy((e + k) % ne, r).start()

    load_left.wait()
    step = tile_of(width, 256)

    @pl.loop(0, nr)
    def _(g):
        columns = pl.ds(pl.multiple_of(g * group, group), group)

        @pl.loop(0, width // step)
        def _(i):
            part = pl.ds(pl.multiple_of(i * step, step), step)
            x[part, columns] = lax.dot_general(
                left[part, :], tok[columns, :], (((1,), (1,)), ((), ())),
                preferred_element_type=jnp.float32,
            ).astype(x.dtype)

    store_x = pltpu.make_async_copy(x, x_ref, local.at[2])
    store_x.start()
    load_right.wait()
    own_cot.wait()

    def store_y(g):
        at = pl.ds(pl.multiple_of(g * group, group), group)
        return pltpu.make_async_copy(y.at[at], y_ref.at[at], local.at[4 + g])

    @pl.loop(0, nr)
    def _(i):
        g = (r + nr // 2 + i) % nr

        @pl.loop(0, ne)
        def _(s):
            @pl.when((s != e) | (g != r))
            def _():
                pltpu.make_async_remote_copy(
                    cot_ref.at[own_rows(s), own_cols(g)], cot.at[span(g, s)],
                    cot_send.at[0], cot_recv.at[g * ne + s],
                    device_id={"expert": (e + 1) % ne, "replica": r},
                ).wait_recv()

        at = pl.ds(pl.multiple_of(g * group, group), group)
        for b in range(blocks):
            inside = slice(b * order, (b + 1) * order)
            y[at, inside] = jnp.dot(
                cot[at, inside], right[b], preferred_element_type=jnp.float32
            ).astype(y.dtype)
        store_y(g).start()

    @pl.loop(1, ne)
    def _(k):
        plane_copy((e + k) % ne).wait_send()

    @pl.loop(0, ne * nr)
    def _(k):
        tr, te = k // ne, k % ne

        @pl.when((te != e) | (tr != r))
        def _():
            cot_copy(te, tr).wait_send()

        @pl.when((tr <= r) & (r + 1 < nr))
        def _():
            relay(tr, te, True).wait_send()

        @pl.when((tr >= r) & (r > 0))
        def _():
            relay(tr, te, False).wait_send()

    store_x.wait()

    @pl.loop(0, nr)
    def _(g):
        store_y(g).wait()


def body(tokens_in, cotangents, left_root, right_root):
    ne, nr = lax.axis_size("expert"), lax.axis_size("replica")
    assert left_root.shape[0] == 1
    width = tokens_in.shape[1]
    columns = cotangents.shape[1] // nr
    total = tokens_in.shape[0] * nr
    blocks, order = right_root.shape[1], right_root.shape[2]
    anywhere = pl.BlockSpec(memory_space=pl.ANY)
    n = ne * nr
    dtype = jnp.bfloat16
    dma = pltpu.SemaphoreType.DMA
    x, y = pl.pallas_call(
        functools.partial(route_kernel, ne, nr),
        out_shape=[
            jax.ShapeDtypeStruct((width, total), dtype),
            jax.ShapeDtypeStruct((total, columns), dtype),
        ],
        in_specs=[anywhere] * 4,
        out_specs=[anywhere] * 2,
        scratch_shapes=[
            pltpu.VMEM((total, width), dtype),
            pltpu.VMEM((total, columns), dtype),
            pltpu.VMEM((width, width), dtype),
            pltpu.VMEM((blocks, order, order), dtype),
            pltpu.VMEM((width, total), dtype),
            pltpu.VMEM((total, columns), dtype),
            dma((ne,)), dma((n,)), dma((n,)), dma((n,)), dma((n,)), dma((n,)), dma((4 + nr,)),
        ],
        compiler_params=pltpu.CompilerParams(collective_id=0, has_side_effects=True),
    )(tokens_in, cotangents, left_root[0], right_root[0])
    return jnp.dot(x, y, preferred_element_type=jnp.float32).astype(dtype)[None]


def solution(mesh):
    in_specs = (
        P(("expert", "replica"), None),
        P(("expert", "replica"), None),
        P("expert", None, None),
        P("expert", "replica", None, None),
    )
    out_specs = P("expert", None, "replica")
    return jax.shard_map(body, mesh=mesh, in_specs=in_specs, out_specs=out_specs, check_vma=False)
```

```python
import functools
import jax
import jax.numpy as jnp
from jax import lax
from jax.experimental import pallas as pl
from jax.experimental.pallas import tpu as pltpu
from jax.sharding import PartitionSpec as P


def tile_of(size, most):
    return most if size % most == 0 else size


def route_kernel(
    ne, nr, tok_ref, cot_ref, left_ref, right_ref, x_ref, y_ref,
    tok, cot, left, right, x, y,
    plane_send, up_send, down_send, tok_recv, cot_send, cot_recv, local,
):
    e = lax.axis_index("expert")
    r = lax.axis_index("replica")
    rows = tok_ref.shape[0] // ne
    group = rows * ne
    width = tok.shape[1]
    cols = cot.shape[1]
    blocks, order = right_ref.shape[0], right_ref.shape[1]

    load_left = pltpu.make_async_copy(left_ref, left, local.at[0])
    load_right = pltpu.make_async_copy(right_ref, right, local.at[1])
    load_left.start()
    load_right.start()

    barrier = pltpu.get_barrier_semaphore()

    @pl.loop(1, ne * nr)
    def _(k):
        pl.semaphore_signal(
            barrier, inc=1,
            device_id={"expert": (e + k % ne) % ne, "replica": (r + k // ne) % nr},
        )

    pl.semaphore_wait(barrier, ne * nr - 1)

    def span(origin, source):
        return pl.ds(pl.multiple_of((origin * ne + source) * rows, rows), rows)

    def own_rows(target):
        return pl.ds(pl.multiple_of(target * rows, rows), rows)

    def own_cols(target):
        return pl.ds(pl.multiple_of(target * cols, cols), cols)

    def plane_copy(target):
        return pltpu.make_async_remote_copy(
            tok_ref.at[own_rows(target)], tok.at[span(r, e)],
            plane_send.at[target], tok_recv.at[r * ne + e],
            device_id={"expert": target, "replica": r},
        )

    def relay(origin, source, up):
        at = span(origin, source)
        k = origin * ne + source
        return pltpu.make_async_remote_copy(
            tok.at[at], tok.at[at],
            (up_send if up else down_send).at[k], tok_recv.at[k],
            device_id={"expert": e, "replica": r + 1 if up else r - 1},
        )

    def tok_wait(origin, source):
        pltpu.make_async_remote_copy(
            tok.at[span(origin, source)], tok.at[span(origin, source)],
            up_send.at[0], tok_recv.at[origin * ne + source],
            device_id={"expert": e, "replica": (r + 1) % nr},
        ).wait_recv()

    def cot_copy(te, tr):
        return pltpu.make_async_remote_copy(
            cot_ref.at[own_rows(te), own_cols(tr)], cot.at[span(r, e)],
            cot_send.at[tr * ne + te], cot_recv.at[r * ne + e],
            device_id={"expert": te, "replica": tr},
        )

    def send_cots(te, distance):
        for tr in (r + distance, r - distance):
            @pl.when((tr >= 0) & (tr < nr))
            def _():
                cot_copy(te, tr).start()

    def forward(origin, source, up):
        ahead = (r + 1 < nr) if up else (r > 0)

        @pl.when(ahead)
        def _():
            relay(origin, source, up).start()

    own_tok = pltpu.make_async_copy(tok_ref.at[own_rows(e)], tok.at[span(r, e)], local.at[2])
    own_cot = pltpu.make_async_copy(cot_ref.at[own_rows(e), own_cols(r)], cot.at[span(r, e)], local.at[3])
    own_tok.start()
    own_cot.start()

    @pl.loop(1, ne)
    def _(k):
        plane_copy((e + k) % ne).start()

    own_tok.wait()

    @pl.loop(0, ne)
    def _(k):
        source = (e + ne - k) % ne

        @pl.when(k > 0)
        def _():
            tok_wait(r, source)

        forward(r, source, True)
        forward(r, source, False)
        for distance in range(nr - 1, 1, -1):
            send_cots((e + k) % ne, distance)

    step = tile_of(width, 256)

    def make_x(g):
        columns = pl.ds(pl.multiple_of(g * group, group), group)

        @pl.loop(0, width // step)
        def _(i):
            part = pl.ds(pl.multiple_of(i * step, step), step)
            x[part, columns] = lax.dot_general(
                left[part, :], tok[columns, :], (((1,), (1,)), ((), ())),
                preferred_element_type=jnp.float32,
            ).astype(x.dtype)

    for distance in range(1, nr):
        @pl.loop(0, ne)
        def _(k):
            source = (e + ne - k) % ne

            @pl.when(r - distance >= 0)
            def _():
                tok_wait(r - distance, source)
                forward(r - distance, source, True)

            @pl.when(r + distance < nr)
            def _():
                tok_wait(r + distance, source)
                forward(r + distance, source, False)

            if distance == 1:
                send_cots((e + k) % ne, 1)

                @pl.when(k > 0)
                def _():
                    cot_copy((e + k) % ne, r).start()

        if distance == 1:
            load_left.wait()
            make_x(r)
        for g in (r - distance, r + distance):
            @pl.when((g >= 0) & (g < nr))
            def _():
                make_x(g)

    store_x = pltpu.make_async_copy(x, x_ref, local.at[2])
    store_x.start()
    load_right.wait()
    own_cot.wait()

    def store_y(g):
        at = pl.ds(pl.multiple_of(g * group, group), group)
        return pltpu.make_async_copy(y.at[at], y_ref.at[at], local.at[4 + g])

    @pl.loop(0, nr)
    def _(i):
        g = (r + nr // 2 + i) % nr

        @pl.loop(0, ne)
        def _(s):
            @pl.when((s != e) | (g != r))
            def _():
                pltpu.make_async_remote_copy(
                    cot_ref.at[own_rows(s), own_cols(g)], cot.at[span(g, s)],
                    cot_send.at[0], cot_recv.at[g * ne + s],
                    device_id={"expert": (e + 1) % ne, "replica": r},
                ).wait_recv()

        at = pl.ds(pl.multiple_of(g * group, group), group)
        for b in range(blocks):
            inside = slice(b * order, (b + 1) * order)
            y[at, inside] = jnp.dot(
                cot[at, inside], right[b], preferred_element_type=jnp.float32
            ).astype(y.dtype)
        store_y(g).start()

    @pl.loop(1, ne)
    def _(k):
        plane_copy((e + k) % ne).wait_send()

    @pl.loop(0, ne * nr)
    def _(k):
        tr, te = k // ne, k % ne

        @pl.when((te != e) | (tr != r))
        def _():
            cot_copy(te, tr).wait_send()

        @pl.when((tr <= r) & (r + 1 < nr))
        def _():
            relay(tr, te, True).wait_send()

        @pl.when((tr >= r) & (r > 0))
        def _():
            relay(tr, te, False).wait_send()

    store_x.wait()

    @pl.loop(0, nr)
    def _(g):
        store_y(g).wait()


def body(tokens_in, cotangents, left_root, right_root):
    ne, nr = lax.axis_size("expert"), lax.axis_size("replica")
    assert left_root.shape[0] == 1
    width = tokens_in.shape[1]
    columns = cotangents.shape[1] // nr
    total = tokens_in.shape[0] * nr
    blocks, order = right_root.shape[1], right_root.shape[2]
    anywhere = pl.BlockSpec(memory_space=pl.ANY)
    n = ne * nr
    dtype = jnp.bfloat16
    dma = pltpu.SemaphoreType.DMA
    x, y = pl.pallas_call(
        functools.partial(route_kernel, ne, nr),
        out_shape=[
            jax.ShapeDtypeStruct((width, total), dtype),
            jax.ShapeDtypeStruct((total, columns), dtype),
        ],
        in_specs=[anywhere] * 4,
        out_specs=[anywhere] * 2,
        scratch_shapes=[
            pltpu.VMEM((total, width), dtype),
            pltpu.VMEM((total, columns), dtype),
            pltpu.VMEM((width, width), dtype),
            pltpu.VMEM((blocks, order, order), dtype),
            pltpu.VMEM((width, total), dtype),
            pltpu.VMEM((total, columns), dtype),
            dma((ne,)), dma((n,)), dma((n,)), dma((n,)), dma((n,)), dma((n,)), dma((4 + nr,)),
        ],
        compiler_params=pltpu.CompilerParams(collective_id=0, has_side_effects=True),
    )(tokens_in, cotangents, left_root[0], right_root[0])
    return jnp.dot(x, y, preferred_element_type=jnp.float32).astype(dtype)[None]


def solution(mesh):
    in_specs = (
        P(("expert", "replica"), None),
        P(("expert", "replica"), None),
        P("expert", None, None),
        P("expert", "replica", None, None),
    )
    out_specs = P("expert", None, "replica")
    return jax.shard_map(body, mesh=mesh, in_specs=in_specs, out_specs=out_specs, check_vma=False)
```
